32 devices in a mesh: section: 4 (over y, core), replica: 8 (over z, x).
Axes of the slice: x: 2, y: 2, z: 4, core: 2. Of those that a mesh axis runs over, the one named last changes fastest.
Arguments:
- gradient: bfloat16 [512, 32768], P('section', 'replica'), may hold values from -1300 to 1300
- residual: float32 [512, 32768], P('section', 'replica'), may hold values from -6 to 6
- block_ids: int32 [4, 64], P('section', 'replica'), may hold values from 0 to 15, as said below
- block_counts: int32 [4, 8], P('section', 'replica'), may hold values from 1 to 8, as said below
Outputs:
- new_residual: float32 [512, 32768], P('section', 'replica')
- update: bfloat16 [512, 4096], P('section', 'replica')
The draws below stay inside these ranges and needn't reach their ends.
Inputs may be any that keep to these rules, and one draw needn't show every extreme that they name: `block_ids`: each device's 8 block numbers are distinct; only the first block_counts of them are selected. `block_counts`: in every section some replica selects exactly 8 blocks; the others select at most 4.
All inputs are finite; a program needn't handle non-finite values.
Results may differ from the reference program's by a relative error of at most 0.013.
Values may be sent and summed in bfloat16 or wider, within the bound.
A program may use at most 64 MiB of HBM per device.

```python
import math
import jax
import jax.numpy as jnp
from jax import lax

D = 4096
ROWS = 128
BLK = 8
KMAX = 8
SECTIONS = 4
REPLICAS = 8


def draw_gradient(key, part):
    key_rows, key_base, key_common, key_level, key_mix, key_slice, key_column = jax.random.split(key, 7)
    slice_width = D // REPLICAS
    row_scale = jnp.exp(jax.random.uniform(key_rows, (SECTIONS * ROWS, REPLICAS, 1), jnp.float32, 0.0, math.log(10.0)))
    section_of_row = (jnp.arange(SECTIONS * ROWS, dtype=jnp.int32) // ROWS).astype(jnp.int32)
    section_scale = 1.0 + 2.0 * section_of_row.astype(jnp.float32) / max(SECTIONS - 1, 1)
    slice_of_column = (jnp.arange(D, dtype=jnp.int32) // slice_width).astype(jnp.int32)
    slice_scale = jnp.exp(jax.random.uniform(key_slice, (REPLICAS,), jnp.float32, 0.0, math.log(4.0)))
    column_rough = jax.random.uniform(key_column, (D,), jnp.float32, 0.6, 1.4)
    column_scale = slice_scale[slice_of_column] * column_rough
    section_level = jax.random.uniform(key_level, (SECTIONS,), jnp.float32, 0.0, 1.2)
    slice_mix = jax.random.uniform(key_mix, (SECTIONS, REPLICAS), jnp.float32, 0.0, 1.0)
    mix_weight = section_level[:, None] * slice_mix
    weight_grid = mix_weight[section_of_row][:, slice_of_column]
    base_draw = jnp.clip(jax.random.normal(key_base, (SECTIONS * ROWS, REPLICAS, D), jnp.float32), -4.0, 4.0)
    common_part = jnp.clip(jax.random.normal(key_common, (SECTIONS * ROWS, 1, D), jnp.float32), -3.0, 3.0)
    base_draw = base_draw + weight_grid[:, None, :] * common_part
    values = base_draw * row_scale * section_scale[:, None, None] * column_scale[None, None, :]
    return values.reshape(SECTIONS * ROWS, REPLICAS * D).astype(jnp.bfloat16)


def draw_block_ids(key, part):
    block_total = ROWS // BLK
    scores = jax.random.randint(key, (SECTIONS, REPLICAS, block_total), 0, 1 << 20) * block_total + jnp.arange(block_total, dtype=jnp.int32)
    ordering = jnp.argsort(scores, axis=-1, stable=True)
    return ordering[..., :KMAX].reshape(SECTIONS, REPLICAS * KMAX).astype(jnp.int32)


def draw_block_counts(key, part):
    key_base, key_busy = jax.random.split(key)
    base_draw = jax.random.randint(key_base, (SECTIONS, REPLICAS), 1, KMAX // 2 + 1)
    busy_replica = jax.random.randint(key_busy, (SECTIONS, 1), 0, REPLICAS)
    placed = jnp.arange(REPLICAS, dtype=jnp.int32)[None, :] == busy_replica
    return jnp.where(placed, KMAX, base_draw).astype(jnp.int32)


def block_scale(stream_key, extent, cuts, low, top_value):
    level, own = 1.0, jax.random.fold_in(stream_key, 6)
    for axis_at, shards_of in cuts:
        draws = jnp.exp(jax.random.uniform(jax.random.fold_in(own, axis_at), (shards_of,), jnp.float32, low / len(cuts), top_value / len(cuts)))
        level = level * jnp.repeat(draws, extent[axis_at] // shards_of).reshape([-1 if axis == axis_at else 1 for axis in range(len(extent))])
    return level


def centred(rng, dims, scale, reach, shards=(), kind=jnp.bfloat16):
    array = scale * jax.random.normal(rng, dims, jnp.float32)
    if shards:
        array = array * block_scale(rng, dims, shards, -0.22, 0.18)
    return jnp.clip(array, -reach, reach).astype(kind)


def setup_inputs(seed: int = 0) -> dict:
    streams_of = jax.random.split(jax.random.key(seed), 5)
    gradient = draw_gradient(jax.random.fold_in(streams_of[4], 71), 0)
    residual = centred(streams_of[1], (SECTIONS * ROWS, REPLICAS * D), 1.0, 6.0, ((0, 4), (1, 8)), jnp.float32)
    block_ids = draw_block_ids(jax.random.fold_in(streams_of[4], 71), 0)
    block_counts = draw_block_counts(jax.random.fold_in(streams_of[4], 71), 0)
    return dict(gradient=gradient, residual=residual, block_ids=block_ids, block_counts=block_counts)


scale_level = 1.0
epsilon = 1e-06

def reference(gradient, residual, block_ids, block_counts):
    block_total = ROWS // BLK
    accumulated = gradient.astype(jnp.float32) + residual
    slot_ids = block_ids.reshape(SECTIONS, REPLICAS, KMAX)
    live_slot = jnp.arange(KMAX, dtype=jnp.int32)[None, None, :] < block_counts[:, :, None]
    hit_table = (slot_ids[..., None] == jnp.arange(block_total, dtype=jnp.int32)) & live_slot[..., None]
    chosen = jnp.any(hit_table, axis=2)
    block_mask = jnp.transpose(chosen, (0, 2, 1))[:, :, None, :, None]
    shaped = accumulated.reshape(SECTIONS, block_total, BLK, REPLICAS, D)
    sent = jnp.where(block_mask, shaped.astype(jnp.bfloat16).astype(jnp.float32), jnp.float32(0.0))
    new_residual = (shaped - sent).reshape(accumulated.shape)
    summed = lax.optimization_barrier(jnp.sum(sent, axis=3)).reshape(SECTIONS * ROWS, D)
    norm_total = jnp.sum(summed * summed)
    root_mean = jnp.sqrt(norm_total / (SECTIONS * ROWS * D) + epsilon)
    clip_factor = scale_level / root_mean
    update = (summed * clip_factor).astype(jnp.bfloat16)
    return (new_residual, update)
```

```python
import functools

import jax
import jax.numpy as jnp
from jax import lax
from jax.experimental import pallas as pl
from jax.experimental.pallas import tpu as pltpu
from jax.sharding import PartitionSpec as P

BLK = 8
CHUNKS = 4
LANES = 128
MESH = pl.DeviceIdType.MESH

scale_level = 1.0
epsilon = 1e-06


def kernel(
    sections,
    replicas,
    ids_ref,
    counts_ref,
    gradient_ref,
    residual_ref,
    update_ref,
    grad_buf,
    acc_buf,
    packed,
    received,
    target_row,
    targets,
    square_row,
    squares,
    load_sems,
    send_sems,
    recv_sems,
    tsend_sems,
    trecv_sems,
    norm_send,
    norm_recv,
):
    row_count, width = gradient_ref.shape
    block_total = row_count // BLK
    slot_count = ids_ref.shape[1]
    slot_rows = slot_count * BLK
    col_count = width // replicas
    section = lax.axis_index("section")
    replica = lax.axis_index("replica")
    total = sections * replicas
    me = section * replicas + replica

    step = row_count // CHUNKS
    loads = []
    for c in range(CHUNKS):
        rows = pl.ds(c * step, step)
        blocks = pl.ds(c * step // BLK, step // BLK)
        one = pltpu.make_async_copy(gradient_ref.at[rows], grad_buf.at[rows], load_sems.at[0, c])
        two = pltpu.make_async_copy(residual_ref.at[blocks], acc_buf.at[blocks], load_sems.at[1, c])
        one.start()
        two.start()
        loads.append((one, two))

    barrier = pltpu.get_barrier_semaphore()

    def greet(k, carry):
        there = lax.rem(me + k, total)
        pl.semaphore_signal(
            barrier,
            inc=1,
            device_id={"section": there // replicas, "replica": lax.rem(there, replicas)},
            device_id_type=MESH,
        )
        return carry

    lax.fori_loop(1, total, greet, 0)

    lane = lax.broadcasted_iota(jnp.int32, (1, LANES), 1)
    row = jnp.full((1, LANES), -1, jnp.int32)
    for s in range(slot_count):
        base = jnp.where(s < counts_ref[0, 0], ids_ref[0, s] * BLK, -2 * row_count)
        row = jnp.where(lane // BLK == s, base + lane % BLK, row)
    target_row[...] = row

    for c in range(CHUNKS):
        for copy in loads[c]:
            copy.wait()
        rows = pl.ds(c * step, step)
        blocks = pl.ds(c * step // BLK, step // BLK)
        value = grad_buf[rows].astype(jnp.float32).reshape(step // BLK, BLK, width)
        acc_buf[blocks] = acc_buf[blocks] + value

    for s in range(0, slot_count, 2):
        pair = jnp.concatenate([acc_buf[ids_ref[0, s]], acc_buf[ids_ref[0, s + 1]]], axis=0)
        pair = pair.astype(jnp.bfloat16)
        for p in range(replicas):
            packed[p, pl.ds(s * BLK, 2 * BLK), :] = pair[:, p * col_count : (p + 1) * col_count]

    pl.semaphore_wait(barrier, total - 1)

    copies = []
    for k in range(1, replicas):
        peer = lax.rem(replica + k, replicas)
        tcopy = pltpu.make_async_remote_copy(
            src_ref=target_row,
            dst_ref=targets.at[k - 1],
            send_sem=tsend_sems.at[k - 1],
            recv_sem=trecv_sems.at[k - 1],
            device_id={"replica": peer},
            device_id_type=MESH,
        )
        copy = pltpu.make_async_remote_copy(
            src_ref=packed.at[peer],
            dst_ref=received.at[k - 1],
            send_sem=send_sems.at[k - 1],
            recv_sem=recv_sems.at[k - 1],
            device_id={"replica": peer},
            device_id_type=MESH,
        )
        tcopy.start()
        copy.start()
        copies.append((tcopy, copy))

    row_iota = lax.broadcasted_iota(jnp.int32, (row_count, slot_rows), 0)

    def place(wanted, block):
        hot = jnp.where(row_iota == wanted, 1.0, 0.0).astype(jnp.bfloat16)
        return jnp.dot(hot, block, preferred_element_type=jnp.float32)

    summed = place(target_row[:, :slot_rows], packed[replica])
    for k in range(1, replicas):
        tcopy, copy = copies[k - 1]
        tcopy.wait_recv()
        copy.wait_recv()
        summed = summed + place(targets[k - 1][:, :slot_rows], received[k - 1])

    lanes = jnp.sum(summed * summed, axis=0, keepdims=True)
    part = lanes[:, :LANES]
    for j in range(1, col_count // LANES):
        part = part + lanes[:, j * LANES : (j + 1) * LANES]
    square_row[...] = part

    def norm_copy(k):
        there = lax.rem(me + k, total)
        return pltpu.make_async_remote_copy(
            src_ref=square_row,
            dst_ref=squares.at[k - 1],
            send_sem=norm_send,
            recv_sem=norm_recv,
            device_id={"section": there // replicas, "replica": lax.rem(there, replicas)},
            device_id_type=MESH,
        )

    def tell(k, carry):
        norm_copy(k).start()
        return carry

    lax.fori_loop(1, total, tell, 0)
    for tcopy, copy in copies:
        tcopy.wait_send()
        copy.wait_send()
    pltpu.make_async_copy(squares, squares, norm_recv).wait()
    pltpu.make_async_copy(squares, squares, norm_send).wait()
    norm_total = jnp.sum(part + jnp.sum(squares[...], axis=0), axis=1, keepdims=True)
    element_count = sections * row_count * width
    root_mean = jnp.sqrt(norm_total / element_count + epsilon)
    clip_factor = scale_level / root_mean
    update_ref[...] = (summed * clip_factor).astype(jnp.bfloat16)


def per_device(sections, replicas, gradient, residual, block_ids, block_counts):
    row_count, width = gradient.shape
    block_total = row_count // BLK
    slot_count = block_ids.shape[1]
    col_count = width // replicas
    total = sections * replicas
    slot_rows = slot_count * BLK
    update = pl.pallas_call(
        functools.partial(kernel, sections, replicas),
        out_shape=jax.ShapeDtypeStruct((row_count, col_count), jnp.bfloat16),
        in_specs=[
            pl.BlockSpec(memory_space=pltpu.SMEM),
            pl.BlockSpec(memory_space=pltpu.SMEM),
            pl.BlockSpec(memory_space=pl.ANY),
            pl.BlockSpec(memory_space=pl.ANY),
        ],
        out_specs=pl.BlockSpec(memory_space=pltpu.VMEM),
        scratch_shapes=[
            pltpu.VMEM((row_count, width), jnp.bfloat16),
            pltpu.VMEM((block_total, BLK, width), jnp.float32),
            pltpu.VMEM((replicas, slot_rows, col_count), jnp.bfloat16),
            pltpu.VMEM((replicas - 1, slot_rows, col_count), jnp.bfloat16),
            pltpu.VMEM((1, LANES), jnp.int32),
            pltpu.VMEM((replicas - 1, 1, LANES), jnp.int32),
            pltpu.VMEM((1, LANES), jnp.float32),
            pltpu.VMEM((total - 1, 1, LANES), jnp.float32),
            pltpu.SemaphoreType.DMA((2, CHUNKS)),
            pltpu.SemaphoreType.DMA((replicas - 1,)),
            pltpu.SemaphoreType.DMA((replicas - 1,)),
            pltpu.SemaphoreType.DMA((replicas - 1,)),
            pltpu.SemaphoreType.DMA((replicas - 1,)),
            pltpu.SemaphoreType.DMA,
            pltpu.SemaphoreType.DMA,
        ],
        compiler_params=pltpu.CompilerParams(collective_id=0, has_side_effects=True),
    )(block_ids, block_counts, gradient, residual.reshape(block_total, BLK, width))

    accumulated = gradient.astype(jnp.float32) + residual
    live_slot = jnp.arange(slot_count, dtype=jnp.int32) < block_counts[0, 0]
    owner = jnp.arange(row_count, dtype=jnp.int32) // BLK
    row_chosen = jnp.any((owner[:, None] == block_ids) & live_slot[None, :], axis=1, keepdims=True)
    sent = jnp.where(
        row_chosen, accumulated.astype(jnp.bfloat16).astype(jnp.float32), jnp.float32(0.0)
    )
    return (accumulated - sent, update)


def solution(mesh):
    spec = P("section", "replica")
    sizes = (mesh.shape["section"], mesh.shape["replica"])
    return jax.shard_map(
        functools.partial(per_device, *sizes),
        mesh=mesh,
        in_specs=(spec,) * 4,
        out_specs=(spec, spec),
        check_vma=False,
    )
```

```python
import functools

import jax
import jax.numpy as jnp
from jax import lax
from jax.experimental import pallas as pl
from jax.experimental.pallas import tpu as pltpu
from jax.sharding import PartitionSpec as P

BLK = 8
CHUNKS = 4
LANES = 128
MESH = pl.DeviceIdType.MESH

scale_level = 1.0
epsilon = 1e-06


def kernel(
    sections,
    replicas,
    ids_ref,
    counts_ref,
    gradient_ref,
    residual_ref,
    update_ref,
    left_ref,
    grad_buf,
    acc_buf,
    packed,
    received,
    target_row,
    targets,
    square_row,
    squares,
    load_sems,
    send_sems,
    recv_sems,
    tsend_sems,
    trecv_sems,
    norm_send,
    norm_recv,
):
    row_count, width = gradient_ref.shape
    block_total = row_count // BLK
    slot_count = ids_ref.shape[1]
    slot_rows = slot_count * BLK
    col_count = width // replicas
    section = lax.axis_index("section")
    replica = lax.axis_index("replica")
    total = sections * replicas

    def ahead(here, extent):
        return [here] + [
            jnp.where(here + k >= extent, here + k - extent, here + k) for k in range(1, extent)
        ]

    section_at = ahead(section, sections)
    replica_at = ahead(replica, replicas)
    others = [(i, j) for i in range(sections) for j in range(replicas) if i + j > 0]

    step = row_count // CHUNKS
    loads = []
    for c in range(CHUNKS):
        rows = pl.ds(c * step, step)
        blocks = pl.ds(c * step // BLK, step // BLK)
        one = pltpu.make_async_copy(gradient_ref.at[rows], grad_buf.at[rows], load_sems.at[0, c])
        two = pltpu.make_async_copy(residual_ref.at[blocks], acc_buf.at[blocks], load_sems.at[1, c])
        one.start()
        two.start()
        loads.append((one, two))

    barrier = pltpu.get_barrier_semaphore()

    for i, j in others:
        pl.semaphore_signal(
            barrier,
            inc=1,
            device_id={"section": section_at[i], "replica": replica_at[j]},
            device_id_type=MESH,
        )

    lane = lax.broadcasted_iota(jnp.int32, (1, LANES), 1)
    row = jnp.full((1, LANES), -1, jnp.int32)
    for s in range(slot_count):
        base = jnp.where(s < counts_ref[0, 0], ids_ref[0, s] * BLK, -2 * row_count)
        row = jnp.where(lane // BLK == s, base + lane % BLK, row)
    target_row[...] = row

    for c in range(CHUNKS):
        for copy in loads[c]:
            copy.wait()
        rows = pl.ds(c * step, step)
        blocks = pl.ds(c * step // BLK, step // BLK)
        value = grad_buf[rows].astype(jnp.float32).reshape(step // BLK, BLK, width)
        acc_buf[blocks] = acc_buf[blocks] + value

    for s in range(0, slot_count, 2):
        pair = jnp.concatenate([acc_buf[ids_ref[0, s]], acc_buf[ids_ref[0, s + 1]]], axis=0)
        pair = pair.astype(jnp.bfloat16)
        for p in range(replicas):
            packed[p, pl.ds(s * BLK, 2 * BLK), :] = pair[:, p * col_count : (p + 1) * col_count]

    pl.semaphore_wait(barrier, total - 1)

    copies = []
    for k in range(1, replicas):
        peer = replica_at[k]
        tcopy = pltpu.make_async_remote_copy(
            src_ref=target_row,
            dst_ref=targets.at[k - 1],
            send_sem=tsend_sems.at[k - 1],
            recv_sem=trecv_sems.at[k - 1],
            device_id={"replica": peer},
            device_id_type=MESH,
        )
        copy = pltpu.make_async_remote_copy(
            src_ref=packed.at[peer],
            dst_ref=received.at[k - 1],
            send_sem=send_sems.at[k - 1],
            recv_sem=recv_sems.at[k - 1],
            device_id={"replica": peer},
            device_id_type=MESH,
        )
        tcopy.start()
        copy.start()
        copies.append((tcopy, copy))

    for c in range(CHUNKS):
        for b in range(c * step // BLK, (c + 1) * step // BLK):
            chosen = jnp.int32(0)
            for s in range(slot_count):
                hit = (ids_ref[0, s] == b) & (s < counts_ref[0, 0])
                chosen = jnp.where(hit, 1, chosen)
            value = acc_buf[b]
            rounded = value.astype(jnp.bfloat16).astype(jnp.float32)
            left_ref[b] = value - jnp.where(chosen > 0, rounded, 0.0)

    row_iota = lax.broadcasted_iota(jnp.int32, (row_count, slot_rows), 0)

    def place(wanted, block):
        hot = jnp.where(row_iota == wanted, 1.0, 0.0).astype(jnp.bfloat16)
        return jnp.dot(hot, block, preferred_element_type=jnp.float32)

    summed = place(target_row[:, :slot_rows], packed[replica])
    for k in range(1, replicas):
        tcopy, copy = copies[k - 1]
        tcopy.wait_recv()
        copy.wait_recv()
        summed = summed + place(targets[k - 1][:, :slot_rows], received[k - 1])

    lanes = jnp.sum(summed * summed, axis=0, keepdims=True)
    part = lanes[:, :LANES]
    for j in range(1, col_count // LANES):
        part = part + lanes[:, j * LANES : (j + 1) * LANES]
    square_row[...] = part

    for slot, (i, j) in enumerate(others):
        pltpu.make_async_remote_copy(
            src_ref=square_row,
            dst_ref=squares.at[slot],
            send_sem=norm_send,
            recv_sem=norm_recv,
            device_id={"section": section_at[i], "replica": replica_at[j]},
            device_id_type=MESH,
        ).start()
    for tcopy, copy in copies:
        tcopy.wait_send()
        copy.wait_send()
    pltpu.make_async_copy(squares, squares, norm_recv).wait()
    pltpu.make_async_copy(squares, squares, norm_send).wait()
    norm_total = jnp.sum(part + jnp.sum(squares[...], axis=0), axis=1, keepdims=True)
    element_count = sections * row_count * width
    root_mean = jnp.sqrt(norm_total / element_count + epsilon)
    clip_factor = scale_level / root_mean
    update_ref[...] = (summed * clip_factor).astype(jnp.bfloat16)


def per_device(sections, replicas, gradient, residual, block_ids, block_counts):
    row_count, width = gradient.shape
    block_total = row_count // BLK
    slot_count = block_ids.shape[1]
    col_count = width // replicas
    total = sections * replicas
    slot_rows = slot_count * BLK
    update, left = pl.pallas_call(
        functools.partial(kernel, sections, replicas),
        out_shape=(
            pltpu.VMEM((row_count, col_count), jnp.bfloat16),
            pltpu.VMEM((block_total, BLK, width), jnp.float32),
        ),
        in_specs=[
            pl.BlockSpec(memory_space=pltpu.SMEM),
            pl.BlockSpec(memory_space=pltpu.SMEM),
            pl.BlockSpec(memory_space=pl.ANY),
            pl.BlockSpec(memory_space=pl.ANY),
        ],
        out_specs=(
            pl.BlockSpec(memory_space=pltpu.VMEM),
            pl.BlockSpec(memory_space=pltpu.VMEM),
        ),
        scratch_shapes=[
            pltpu.VMEM((row_count, width), jnp.bfloat16),
            pltpu.VMEM((block_total, BLK, width), jnp.float32),
            pltpu.VMEM((replicas, slot_rows, col_count), jnp.bfloat16),
            pltpu.VMEM((replicas - 1, slot_rows, col_count), jnp.bfloat16),
            pltpu.VMEM((1, LANES), jnp.int32),
            pltpu.VMEM((replicas - 1, 1, LANES), jnp.int32),
            pltpu.VMEM((1, LANES), jnp.float32),
            pltpu.VMEM((total - 1, 1, LANES), jnp.float32),
            pltpu.SemaphoreType.DMA((2, CHUNKS)),
            pltpu.SemaphoreType.DMA((replicas - 1,)),
            pltpu.SemaphoreType.DMA((replicas - 1,)),
            pltpu.SemaphoreType.DMA((replicas - 1,)),
            pltpu.SemaphoreType.DMA((replicas - 1,)),
            pltpu.SemaphoreType.DMA,
            pltpu.SemaphoreType.DMA,
        ],
        compiler_params=pltpu.CompilerParams(collective_id=0, has_side_effects=True),
    )(block_ids, block_counts, gradient, residual.reshape(block_total, BLK, width))

    return (left.reshape(row_count, width), update)


def solution(mesh):
    spec = P("section", "replica")
    sizes = (mesh.shape["section"], mesh.shape["replica"])
    return jax.shard_map(
        functools.partial(per_device, *sizes),
        mesh=mesh,
        in_specs=(spec,) * 4,
        out_specs=(spec, spec),
        check_vma=False,
    )
```

```python
import functools

import jax
import jax.numpy as jnp
from jax import lax
from jax.experimental import pallas as pl
from jax.experimental.pallas import tpu as pltpu
from jax.sharding import PartitionSpec as P

BLK = 8
CHUNKS = 4
LANES = 128
MESH = pl.DeviceIdType.MESH

scale_level = 1.0
epsilon = 1e-06


def kernel(
    sections,
    replicas,
    ids_ref,
    counts_ref,
    gradient_ref,
    residual_ref,
    update_ref,
    left_ref,
    grad_buf,
    acc_buf,
    packed,
    received,
    target_row,
    targets,
    square_row,
    squares,
    load_sems,
    relayed,
    far_targets,
    far_data,
    cross_buf,
    cross_in,
    relay_sems,
    near_row_sems,
    near_sems,
    far_row_sems,
    far_sems,
    cross_sems,
    norm_send,
    norm_recv,
):
    row_count, width = gradient_ref.shape
    block_total = row_count // BLK
    slot_count = ids_ref.shape[1]
    slot_rows = slot_count * BLK
    cap = slot_count // 2
    cap_rows = cap * BLK
    half = replicas // 2
    col_count = width // replicas
    section = lax.axis_index("section")
    replica = lax.axis_index("replica")
    total = sections * replicas

    def ahead(here, extent):
        return [here] + [
            jnp.where(here + k >= extent, here + k - extent, here + k) for k in range(1, extent)
        ]

    section_at = ahead(section, sections)
    replica_at = ahead(replica, replicas)
    others = [(i, j) for i in range(sections) for j in range(replicas) if i + j > 0]

    step = row_count // CHUNKS
    loads = []
    for c in range(CHUNKS):
        rows = pl.ds(c * step, step)
        blocks = pl.ds(c * step // BLK, step // BLK)
        one = pltpu.make_async_copy(gradient_ref.at[rows], grad_buf.at[rows], load_sems.at[0, c])
        two = pltpu.make_async_copy(residual_ref.at[blocks], acc_buf.at[blocks], load_sems.at[1, c])
        one.start()
        two.start()
        loads.append((one, two))

    barrier = pltpu.get_barrier_semaphore()

    for i, j in others:
        pl.semaphore_signal(
            barrier,
            inc=1,
            device_id={"section": section_at[i], "replica": replica_at[j]},
            device_id_type=MESH,
        )

    lane = lax.broadcasted_iota(jnp.int32, (1, LANES), 1)
    row = jnp.full((1, LANES), -1, jnp.int32)
    for s in range(slot_count):
        base = jnp.where(s < counts_ref[0, 0], ids_ref[0, s] * BLK, -2 * row_count)
        row = jnp.where(lane // BLK == s, base + lane % BLK, row)
    target_row[...] = row

    for c in range(CHUNKS):
        for copy in loads[c]:
            copy.wait()
        rows = pl.ds(c * step, step)
        blocks = pl.ds(c * step // BLK, step // BLK)
        value = grad_buf[rows].astype(jnp.float32).reshape(step // BLK, BLK, width)
        acc_buf[blocks] = acc_buf[blocks] + value

    for s in range(0, slot_count, 2):
        pair = [acc_buf[ids_ref[0, s + i]] for i in range(2)]
        if s >= cap:
            pair = [jnp.where(s + i < counts_ref[0, 0], pair[i], 0.0) for i in range(2)]
        pair = jnp.concatenate(pair, axis=0).astype(jnp.bfloat16)
        for p in range(replicas):
            packed[p, pl.ds(s * BLK, 2 * BLK), :] = pair[:, p * col_count : (p + 1) * col_count]

    pl.semaphore_wait(barrier, total - 1)

    side = replica // half * half
    other_side = half - side
    place_in_side = replica - side
    inner = [
        jnp.where(place_in_side + k >= half, place_in_side + k - half, place_in_side + k)
        for k in range(half)
    ]

    def send(src, dst, sems, slot, peer):
        copy = pltpu.make_async_remote_copy(
            src_ref=src,
            dst_ref=dst,
            send_sem=sems.at[0, slot],
            recv_sem=sems.at[1, slot],
            device_id={"replica": peer},
            device_id_type=MESH,
        )
        copy.start()
        return copy

    relay_in, near_rows, near, far_rows, far = {}, {}, {}, {}, {}
    for k in range(half - 1, 0, -1):
        peer = side + inner[k]
        source = packed.at[other_side + inner[k], pl.ds(cap_rows, slot_rows - cap_rows)]
        relay_in[k] = send(source, relayed.at[k - 1], relay_sems, k - 1, peer)
    for k in range(half - 1, -1, -1):
        peer = other_side + inner[k]
        far_rows[k] = send(target_row, far_targets.at[k], far_row_sems, k, peer)
        far[k] = send(packed.at[peer, pl.ds(0, cap_rows)], far_data.at[k], far_sems, k, peer)
    for k in range(half - 1, 0, -1):
        peer = side + inner[k]
        near_rows[k] = send(target_row, targets.at[k - 1], near_row_sems, k - 1, peer)
        near[k] = send(packed.at[peer], received.at[k - 1], near_sems, k - 1, peer)

    for c in range(CHUNKS):
        for b in range(c * step // BLK, (c + 1) * step // BLK):
            chosen = jnp.int32(0)
            for s in range(slot_count):
                hit = (ids_ref[0, s] == b) & (s < counts_ref[0, 0])
                chosen = jnp.where(hit, 1, chosen)
            value = acc_buf[b]
            rounded = value.astype(jnp.bfloat16).astype(jnp.float32)
            left_ref[b] = value - jnp.where(chosen > 0, rounded, 0.0)


    def place(wanted, block):
        row_iota = lax.broadcasted_iota(jnp.int32, (row_count, wanted.shape[1]), 0)
        hot = jnp.where(row_iota == wanted, 1.0, 0.0).astype(jnp.bfloat16)
        return jnp.dot(hot, block, preferred_element_type=jnp.float32)

    crossing = packed[other_side + place_in_side, cap_rows:, :].astype(jnp.float32)
    for k in range(1, half):
        relay_in[k].wait_recv()
        crossing = crossing + relayed[k - 1].astype(jnp.float32)
    cross_buf[...] = crossing.astype(jnp.bfloat16)
    cross = send(cross_buf, cross_in, cross_sems, 0, other_side + place_in_side)

    summed = place(target_row[:, :slot_rows], packed[replica])
    for k in range(1, half):
        near_rows[k].wait_recv()
        near[k].wait_recv()
        summed = summed + place(targets[k - 1][:, :slot_rows], received[k - 1])
    wanted = jnp.full((1, slot_rows), -1, jnp.int32)
    for k in range(half):
        far_rows[k].wait_recv()
        far[k].wait_recv()
        theirs = far_targets[k][:, :slot_rows]
        wanted = jnp.maximum(wanted, theirs)
        summed = summed + place(theirs[:, :cap_rows], far_data[k])
    cross.wait_recv()
    summed = summed + place(wanted[:, cap_rows:], cross_in[...])

    lanes = jnp.sum(summed * summed, axis=0, keepdims=True)
    part = lanes[:, :LANES]
    for j in range(1, col_count // LANES):
        part = part + lanes[:, j * LANES : (j + 1) * LANES]
    square_row[...] = part

    for slot, (i, j) in enumerate(others):
        pltpu.make_async_remote_copy(
            src_ref=square_row,
            dst_ref=squares.at[slot],
            send_sem=norm_send,
            recv_sem=norm_recv,
            device_id={"section": section_at[i], "replica": replica_at[j]},
            device_id_type=MESH,
        ).start()
    for group in (relay_in, near_rows, near, far_rows, far, {0: cross}):
        for copy in group.values():
            copy.wait_send()
    pltpu.make_async_copy(squares, squares, norm_recv).wait()
    pltpu.make_async_copy(squares, squares, norm_send).wait()
    norm_total = jnp.sum(part + jnp.sum(squares[...], axis=0), axis=1, keepdims=True)
    element_count = sections * row_count * width
    root_mean = jnp.sqrt(norm_total / element_count + epsilon)
    clip_factor = scale_level / root_mean
    update_ref[...] = (summed * clip_factor).astype(jnp.bfloat16)


def per_device(sections, replicas, gradient, residual, block_ids, block_counts):
    row_count, width = gradient.shape
    block_total = row_count // BLK
    slot_count = block_ids.shape[1]
    col_count = width // replicas
    total = sections * replicas
    slot_rows = slot_count * BLK
    over_rows = slot_rows - slot_count // 2 * BLK
    half = replicas // 2
    update, left = pl.pallas_call(
        functools.partial(kernel, sections, replicas),
        out_shape=(
            pltpu.VMEM((row_count, col_count), jnp.bfloat16),
            pltpu.VMEM((block_total, BLK, width), jnp.float32),
        ),
        in_specs=[
            pl.BlockSpec(memory_space=pltpu.SMEM),
            pl.BlockSpec(memory_space=pltpu.SMEM),
            pl.BlockSpec(memory_space=pl.ANY),
            pl.BlockSpec(memory_space=pl.ANY),
        ],
        out_specs=(
            pl.BlockSpec(memory_space=pltpu.VMEM),
            pl.BlockSpec(memory_space=pltpu.VMEM),
        ),
        scratch_shapes=[
            pltpu.VMEM((row_count, width), jnp.bfloat16),
            pltpu.VMEM((block_total, BLK, width), jnp.float32),
            pltpu.VMEM((replicas, slot_rows, col_count), jnp.bfloat16),
            pltpu.VMEM((half - 1, slot_rows, col_count), jnp.bfloat16),
            pltpu.VMEM((1, LANES), jnp.int32),
            pltpu.VMEM((half - 1, 1, LANES), jnp.int32),
            pltpu.VMEM((1, LANES), jnp.float32),
            pltpu.VMEM((total - 1, 1, LANES), jnp.float32),
            pltpu.SemaphoreType.DMA((2, CHUNKS)),
            pltpu.VMEM((half - 1, over_rows, col_count), jnp.bfloat16),
            pltpu.VMEM((half, 1, LANES), jnp.int32),
            pltpu.VMEM((half, slot_rows - over_rows, col_count), jnp.bfloat16),
            pltpu.VMEM((over_rows, col_count), jnp.bfloat16),
            pltpu.VMEM((over_rows, col_count), jnp.bfloat16),
            pltpu.SemaphoreType.DMA((2, half - 1)),
            pltpu.SemaphoreType.DMA((2, half - 1)),
            pltpu.SemaphoreType.DMA((2, half - 1)),
            pltpu.SemaphoreType.DMA((2, half)),
            pltpu.SemaphoreType.DMA((2, half)),
            pltpu.SemaphoreType.DMA((2, 1)),
            pltpu.SemaphoreType.DMA,
            pltpu.SemaphoreType.DMA,
        ],
        compiler_params=pltpu.CompilerParams(collective_id=0, has_side_effects=True),
    )(block_ids, block_counts, gradient, residual.reshape(block_total, BLK, width))

    return (left.reshape(row_count, width), update)


def solution(mesh):
    spec = P("section", "replica")
    sizes = (mesh.shape["section"], mesh.shape["replica"])
    return jax.shard_map(
        functools.partial(per_device, *sizes),
        mesh=mesh,
        in_specs=(spec,) * 4,
        out_specs=(spec, spec),
        check_vma=False,
    )
```

```python
import functools

import jax
import jax.numpy as jnp
from jax import lax
from jax.experimental import pallas as pl
from jax.experimental.pallas import tpu as pltpu
from jax.sharding import PartitionSpec as P

BLK = 8
CHUNKS = 4
LANES = 128
MESH = pl.DeviceIdType.MESH

scale_level = 1.0
epsilon = 1e-06


def kernel(
    sections,
    replicas,
    ids_hbm,
    counts_hbm,
    gradient_ref,
    residual_ref,
    update_ref,
    left_ref,
    grad_buf,
    acc_buf,
    packed,
    received,
    target_row,
    targets,
    square_row,
    squares,
    load_sems,
    ids_ref,
    counts_ref,
    list_sems,
    relayed,
    far_targets,
    far_data,
    cross_buf,
    cross_in,
    relay_sems,
    near_row_sems,
    near_sems,
    far_row_sems,
    far_sems,
    cross_sems,
    norm_send,
    norm_recv,
):
    row_count, width = gradient_ref.shape
    block_total = row_count // BLK
    slot_count = ids_hbm.shape[1]
    slot_rows = slot_count * BLK
    cap = slot_count // 2
    cap_rows = cap * BLK
    half = replicas // 2
    col_count = width // replicas
    section = lax.axis_index("section")
    replica = lax.axis_index("replica")
    total = sections * replicas

    def ahead(here, extent):
        return [here] + [
            jnp.where(here + k >= extent, here + k - extent, here + k) for k in range(1, extent)
        ]

    section_at = ahead(section, sections)
    replica_at = ahead(replica, replicas)
    others = [(i, j) for i in range(sections) for j in range(replicas) if i + j > 0]

    lists = [
        pltpu.make_async_copy(ids_hbm, ids_ref, list_sems.at[0]),
        pltpu.make_async_copy(counts_hbm, counts_ref, list_sems.at[1]),
    ]
    for copy in lists:
        copy.start()

    step = row_count // CHUNKS
    loads = []
    for c in range(CHUNKS):
        rows = pl.ds(c * step, step)
        blocks = pl.ds(c * step // BLK, step // BLK)
        one = pltpu.make_async_copy(gradient_ref.at[rows], grad_buf.at[rows], load_sems.at[0, c])
        two = pltpu.make_async_copy(residual_ref.at[blocks], acc_buf.at[blocks], load_sems.at[1, c])
        one.start()
        two.start()
        loads.append((one, two))

    barrier = pltpu.get_barrier_semaphore()

    for i, j in others:
        pl.semaphore_signal(
            barrier,
            inc=1,
            device_id={"section": section_at[i], "replica": replica_at[j]},
            device_id_type=MESH,
        )

    for copy in lists:
        copy.wait()
    lane = lax.broadcasted_iota(jnp.int32, (1, LANES), 1)
    row = jnp.full((1, LANES), -1, jnp.int32)
    for s in range(slot_count):
        base = jnp.where(s < counts_ref[0, 0], ids_ref[0, s] * BLK, -2 * row_count)
        row = jnp.where(lane // BLK == s, base + lane % BLK, row)
    target_row[...] = row

    for c in range(CHUNKS):
        for copy in loads[c]:
            copy.wait()
        rows = pl.ds(c * step, step)
        blocks = pl.ds(c * step // BLK, step // BLK)
        value = grad_buf[rows].astype(jnp.float32).reshape(step // BLK, BLK, width)
        acc_buf[blocks] = acc_buf[blocks] + value

    for s in range(0, slot_count, 2):
        pair = [acc_buf[ids_ref[0, s + i]] for i in range(2)]
        if s >= cap:
            pair = [jnp.where(s + i < counts_ref[0, 0], pair[i], 0.0) for i in range(2)]
        pair = jnp.concatenate(pair, axis=0).astype(jnp.bfloat16)
        for p in range(replicas):
            packed[p, pl.ds(s * BLK, 2 * BLK), :] = pair[:, p * col_count : (p + 1) * col_count]

    pl.semaphore_wait(barrier, total - 1)

    side = replica // half * half
    other_side = half - side
    place_in_side = replica - side
    inner = [
        jnp.where(place_in_side + k >= half, place_in_side + k - half, place_in_side + k)
        for k in range(half)
    ]

    def send(src, dst, sems, slot, peer):
        copy = pltpu.make_async_remote_copy(
            src_ref=src,
            dst_ref=dst,
            send_sem=sems.at[0, slot],
            recv_sem=sems.at[1, slot],
            device_id={"replica": peer},
            device_id_type=MESH,
        )
        copy.start()
        return copy

    relay_in, near_rows, near, far_rows, far = {}, {}, {}, {}, {}
    for k in range(half - 1, 0, -1):
        peer = side + inner[k]
        source = packed.at[other_side + inner[k], pl.ds(cap_rows, slot_rows - cap_rows)]
        relay_in[k] = send(source, relayed.at[k - 1], relay_sems, k - 1, peer)
    for k in range(half - 1, -1, -1):
        peer = other_side + inner[k]
        far_rows[k] = send(target_row, far_targets.at[k], far_row_sems, k, peer)
        far[k] = send(packed.at[peer, pl.ds(0, cap_rows)], far_data.at[k], far_sems, k, peer)
    for k in range(half - 1, 0, -1):
        peer = side + inner[k]
        near_rows[k] = send(target_row, targets.at[k - 1], near_row_sems, k - 1, peer)
        near[k] = send(packed.at[peer], received.at[k - 1], near_sems, k - 1, peer)

    for c in range(CHUNKS):
        for b in range(c * step // BLK, (c + 1) * step // BLK):
            chosen = jnp.int32(0)
            for s in range(slot_count):
                hit = (ids_ref[0, s] == b) & (s < counts_ref[0, 0])
                chosen = jnp.where(hit, 1, chosen)
            value = acc_buf[b]
            rounded = value.astype(jnp.bfloat16).astype(jnp.float32)
            left_ref[b] = value - jnp.where(chosen > 0, rounded, 0.0)


    def place(wanted, block):
        row_iota = lax.broadcasted_iota(jnp.int32, (row_count, wanted.shape[1]), 0)
        hot = jnp.where(row_iota == wanted, 1.0, 0.0).astype(jnp.bfloat16)
        return jnp.dot(hot, block, preferred_element_type=jnp.float32)

    crossing = packed[other_side + place_in_side, cap_rows:, :].astype(jnp.float32)
    for k in range(1, half):
        relay_in[k].wait_recv()
        crossing = crossing + relayed[k - 1].astype(jnp.float32)
    cross_buf[...] = crossing.astype(jnp.bfloat16)
    cross = send(cross_buf, cross_in, cross_sems, 0, other_side + place_in_side)

    summed = place(target_row[:, :slot_rows], packed[replica])
    for k in range(1, half):
        near_rows[k].wait_recv()
        near[k].wait_recv()
        summed = summed + place(targets[k - 1][:, :slot_rows], received[k - 1])
    wanted = jnp.full((1, slot_rows), -1, jnp.int32)
    for k in range(half):
        far_rows[k].wait_recv()
        far[k].wait_recv()
        theirs = far_targets[k][:, :slot_rows]
        wanted = jnp.maximum(wanted, theirs)
        summed = summed + place(theirs[:, :cap_rows], far_data[k])
    cross.wait_recv()
    summed = summed + place(wanted[:, cap_rows:], cross_in[...])

    lanes = jnp.sum(summed * summed, axis=0, keepdims=True)
    part = lanes[:, :LANES]
    for j in range(1, col_count // LANES):
        part = part + lanes[:, j * LANES : (j + 1) * LANES]
    square_row[...] = part

    for slot, (i, j) in enumerate(others):
        pltpu.make_async_remote_copy(
            src_ref=square_row,
            dst_ref=squares.at[slot],
            send_sem=norm_send,
            recv_sem=norm_recv,
            device_id={"section": section_at[i], "replica": replica_at[j]},
            device_id_type=MESH,
        ).start()
    for group in (relay_in, near_rows, near, far_rows, far, {0: cross}):
        for copy in group.values():
            copy.wait_send()
    pltpu.make_async_copy(squares, squares, norm_recv).wait()
    pltpu.make_async_copy(squares, squares, norm_send).wait()
    norm_total = jnp.sum(part + jnp.sum(squares[...], axis=0), axis=1, keepdims=True)
    element_count = sections * row_count * width
    root_mean = jnp.sqrt(norm_total / element_count + epsilon)
    clip_factor = scale_level / root_mean
    update_ref[...] = (summed * clip_factor).astype(jnp.bfloat16)


def per_device(sections, replicas, gradient, residual, block_ids, block_counts):
    row_count, width = gradient.shape
    block_total = row_count // BLK
    slot_count = block_ids.shape[1]
    col_count = width // replicas
    total = sections * replicas
    slot_rows = slot_count * BLK
    over_rows = slot_rows - slot_count // 2 * BLK
    half = replicas // 2
    update, left = pl.pallas_call(
        functools.partial(kernel, sections, replicas),
        out_shape=(
            pltpu.VMEM((row_count, col_count), jnp.bfloat16),
            pltpu.VMEM((block_total, BLK, width), jnp.float32),
        ),
        in_specs=[
            pl.BlockSpec(memory_space=pl.ANY),
            pl.BlockSpec(memory_space=pl.ANY),
            pl.BlockSpec(memory_space=pl.ANY),
            pl.BlockSpec(memory_space=pl.ANY),
        ],
        out_specs=(
            pl.BlockSpec(memory_space=pltpu.VMEM),
            pl.BlockSpec(memory_space=pltpu.VMEM),
        ),
        scratch_shapes=[
            pltpu.VMEM((row_count, width), jnp.bfloat16),
            pltpu.VMEM((block_total, BLK, width), jnp.float32),
            pltpu.VMEM((replicas, slot_rows, col_count), jnp.bfloat16),
            pltpu.VMEM((half - 1, slot_rows, col_count), jnp.bfloat16),
            pltpu.VMEM((1, LANES), jnp.int32),
            pltpu.VMEM((half - 1, 1, LANES), jnp.int32),
            pltpu.VMEM((1, LANES), jnp.float32),
            pltpu.VMEM((total - 1, 1, LANES), jnp.float32),
            pltpu.SemaphoreType.DMA((2, CHUNKS)),
            pltpu.SMEM(block_ids.shape, jnp.int32),
            pltpu.SMEM(block_counts.shape, jnp.int32),
            pltpu.SemaphoreType.DMA((2,)),
            pltpu.VMEM((half - 1, over_rows, col_count), jnp.bfloat16),
            pltpu.VMEM((half, 1, LANES), jnp.int32),
            pltpu.VMEM((half, slot_rows - over_rows, col_count), jnp.bfloat16),
            pltpu.VMEM((over_rows, col_count), jnp.bfloat16),
            pltpu.VMEM((over_rows, col_count), jnp.bfloat16),
            pltpu.SemaphoreType.DMA((2, half - 1)),
            pltpu.SemaphoreType.DMA((2, half - 1)),
            pltpu.SemaphoreType.DMA((2, half - 1)),
            pltpu.SemaphoreType.DMA((2, half)),
            pltpu.SemaphoreType.DMA((2, half)),
            pltpu.SemaphoreType.DMA((2, 1)),
            pltpu.SemaphoreType.DMA,
            pltpu.SemaphoreType.DMA,
        ],
        compiler_params=pltpu.CompilerParams(collective_id=0, has_side_effects=True),
    )(block_ids, block_counts, gradient, residual.reshape(block_total, BLK, width))

    return (left.reshape(row_count, width), update)


def solution(mesh):
    spec = P("section", "replica")
    sizes = (mesh.shape["section"], mesh.shape["replica"])
    return jax.shard_map(
        functools.partial(per_device, *sizes),
        mesh=mesh,
        in_specs=(spec,) * 4,
        out_specs=(spec, spec),
        check_vma=False,
    )
```
